32 devices in a mesh: groups: 2 (over y), seq: 4 (over z), tp: 2 (over x), ref: 2 (over core).
Axes of the slice: x: 2, y: 2, z: 4, core: 2. Of those that a mesh axis runs over, the one named last changes fastest.
Arguments:
- hidden: bfloat16 [2, 2048, 4096], P('ref', ('groups', 'seq'), 'tp'), parts along dimension 1, may hold values from -6 to 6
- segment_ids: int32 [2048], P(('groups', 'seq')), parts along dimension 0, may hold values from 0 to 3, never falling along the last dimension, each value on 1 to 768 neighbouring positions
- targets: int32 [2048], P(('groups', 'seq')), parts along dimension 0, may hold values from 0 to 4095
- loss_mask: int32 [2048], P(('groups', 'seq')), parts along dimension 0, may hold values from 0 to 1, as said below
- attn_gain: float32 [2, 4096], P('ref'), may hold values from 0.5 to 2
- final_gain: float32 [2, 4096], P('ref'), may hold values from 1 to 4
- w_query: bfloat16 [2, 4096, 2048], P('ref', 'seq', 'tp'), may hold values from -0.125 to 0.125
- w_key: bfloat16 [2, 4096, 1024], P('ref', 'seq', 'tp'), may hold values from -0.125 to 0.125
- w_value: bfloat16 [2, 4096, 1024], P('ref', 'seq', 'tp'), may hold values from -0.09375 to 0.09375
- w_out: bfloat16 [2, 2048, 4096], P('ref', 'tp', 'seq'), may hold values from -0.125 to 0.125
- head: bfloat16 [2, 4096, 4096], P('ref', None, ('seq', 'tp')), may hold values from -0.25784398 to 0.25784398
Outputs:
- logprobs: float32 [2, 2048], P('ref', ('groups', 'seq')), parts along dimension 1
The draws below stay inside these ranges and needn't reach their ends.
There are 2 independent parts, one for each index of `groups`. The reference program is written for one: setup_inputs(seed, part) draws one part's arguments, and reference() takes and returns one part's arrays. A program takes and returns all parts, laid end to end along the dimension named above; an argument that names none is the same for every part. Nothing has to cross between parts.
Inputs may be any that keep to these rules, and one draw needn't show every extreme that they name: `loss_mask`: each aligned block of 256 positions holds 1 to 32 positions with mask 1, and some block holds exactly 32. `segment_ids`: never falling; every rollout number appears; the longest rollout holds exactly 768 positions.
All inputs are finite; a program needn't handle non-finite values.
Results may differ from the reference program's by a relative error of at most 0.0003.
Values may be sent and summed in bfloat16 or wider, within the bound.
A program may use at most 128 MiB of HBM per device.

```python
import math
import jax
import jax.numpy as jnp
import numpy as np
from jax import lax

D = 4096
KV_HEADS = 8
HEAD_DIM = 128
HEADS = 16
TOK_DEV = 256
WINDOW = 2048
CAP = 32
SEGMENTS = 4
LENGTH = 1024
VOCAB = 4096


def bounded_normal(key, shape, spread, limit):
    return jnp.clip(jax.random.normal(key, shape, jnp.float32), -limit, limit) * spread


def base_noise(key, shape, spread):
    return bounded_normal(key, shape, spread, 4.0)


def draw_loss_mask(key, part):
    blocks = LENGTH // TOK_DEV
    base = jax.random.fold_in(key, 17)
    first, second, third = jax.random.split(base, 3)
    lowest = max(1, CAP // 4)
    counts = jax.random.randint(first, (blocks,), lowest, CAP + 1)
    fullest = jax.random.randint(second, (), 0, blocks)
    counts = jnp.where(jnp.arange(blocks) == fullest, CAP, counts)
    block_keys = jax.random.split(third, blocks)
    orders = jax.vmap(lambda k: jax.random.permutation(k, TOK_DEV))(block_keys)
    chosen = orders < counts[:, None]
    return chosen.astype(jnp.int32).reshape(LENGTH)


def draw_hidden(key, part):
    noise_key, row_key, height_key = jax.random.split(jax.random.fold_in(key, 31), 3)
    shape = (2, LENGTH, D)
    marked = jax.random.randint(row_key, (LENGTH,), 0, 8) == 0
    height = jax.random.uniform(height_key, (LENGTH,), jnp.float32, 2.0, 4.0)
    noise = bounded_normal(noise_key, shape, 1.0, 6.0)
    drawn = jnp.clip(noise, -4.0, 4.0)
    lifted = jnp.where(marked[None, :, None], 0.5 * drawn + height[None, :, None], noise)
    return lifted.astype(jnp.bfloat16)


def drawn_projection(key, heads):
    noise_key, gain_key = jax.random.split(key)
    columns = heads * HEAD_DIM
    spread = D ** (-0.5)
    noise = base_noise(noise_key, (2, D, columns), spread)
    target = jnp.exp(jax.random.uniform(gain_key, (2, heads, 1), jnp.float32, math.log(150.0), math.log(500.0)))
    strength = jnp.sqrt(target / (0.29 * math.sqrt(HEAD_DIM) * D))
    lanes = jnp.arange(HEAD_DIM) % (HEAD_DIM // 2) >= 3 * HEAD_DIM // 8
    column_lift = (strength * lanes.astype(jnp.float32)[None, None, :]).reshape(2, columns) * spread
    return (noise + column_lift[:, None, :]).astype(jnp.bfloat16)


def draw_w_query(key, part):
    return drawn_projection(jax.random.fold_in(key, 53), HEADS)


def draw_w_key(key, part):
    return drawn_projection(jax.random.fold_in(key, 59), KV_HEADS)


def draw_head(key, part):
    noise_key, pick_key, height_key = jax.random.split(jax.random.fold_in(key, 71), 3)
    spread = (D // 9) ** (-0.5)
    shape = (2, D, VOCAB)
    noise = base_noise(noise_key, shape, spread)
    period = min(256, VOCAB // 8)
    offset = jax.random.randint(pick_key, (2, 1), 0, period)
    place = (jnp.arange(VOCAB)[None, :] + offset) % period
    first = place == 0
    second = place == 1
    height = jax.random.uniform(height_key, (2, VOCAB), jnp.float32, 2.0, 4.0)
    partner = jnp.roll(height, 1, axis=1)
    cut = max(1, math.isqrt(D) // 8)
    kept = (jnp.arange(D) >= cut).astype(jnp.float32)[None, :, None]
    lift_first = (height * spread)[:, None, :]
    lift_second = (partner * spread)[:, None, :] * kept
    planted = jnp.where(first[:, None, :], lift_first + 0.25 * noise, jnp.where(second[:, None, :], lift_second + 0.25 * noise, noise))
    return planted.astype(jnp.bfloat16)


def touch_ends(array, own_key, least, top_value):
    index_at = [jax.random.randint(jax.random.fold_in(own_key, axis), (), 0, length) for axis, length in enumerate(array.shape)]
    longest = array.shape.index(max(array.shape))
    next_to = index_at[:longest] + [(index_at[longest] + 1) % array.shape[longest]] + index_at[longest + 1:]
    return array.at[tuple(index_at)].set(least).at[tuple(next_to)].set(top_value)


def shard_levels(rng, extent, cuts, smallest, top_value):
    level, own = 1.0, jax.random.fold_in(rng, 6)
    for axis_at, parts in cuts:
        heights = jnp.exp(jax.random.uniform(jax.random.fold_in(own, axis_at), (parts,), jnp.float32, smallest / len(cuts), top_value / len(cuts)))
        level = level * jnp.repeat(heights, extent[axis_at] // parts).reshape([-1 if axis == axis_at else 1 for axis in range(len(extent))])
    return level


def rank_bounds(amount, lean):
    portions = [(1 << 20) // math.isqrt(grade ** lean) + 1 for grade in range(1, amount + 1)]
    width = 1 + sum(portions) // (1 << 30)
    return np.cumsum(np.array([max(1, weight // width) for weight in portions]))


def skewed_ids(own_key, extent, count, skew):
    grid = rank_bounds(count, skew)
    pick = jax.random.randint(jax.random.fold_in(own_key, 1), extent, 0, int(grid[count - 1]))
    standing = jnp.searchsorted(jnp.asarray(grid, jnp.int32), pick, side="right")
    return jax.random.permutation(jax.random.fold_in(own_key, 2), count)[standing].astype(jnp.int32)


def length_profile(number_of, total, bound, skew):
    portions = [(1 << 20) // math.isqrt(grade ** skew) + 1 for grade in range(2, number_of + 1)]
    spare, given = total - bound - (number_of - 1), [1] * (number_of - 1)
    while spare > 0:
        free = [i for i in range(number_of - 1) if given[i] < bound]
        whole, left = sum([portions[i] for i in free]), spare
        for i in free:
            extra = min(bound - given[i], max(1, left * portions[i] // whole), spare)
            given[i] = given[i] + extra
            spare = spare - extra
    return np.array([bound] + given)


def uneven_parts(rng, amount, total, reach, lean):
    if amount == 2:
        one = jax.random.randint(rng, (), max(1, total - reach), min(reach, total - 1) + 1)
        return jnp.stack([one, total - one])
    tallies = jnp.asarray(length_profile(amount, total, reach, lean), jnp.int32)
    twos = (amount - 1) // 2
    giver, taker = tallies[1:1 + 2 * twos:2], tallies[2:2 + 2 * twos:2]
    margin = jnp.minimum(giver - 1, reach - taker)
    moved = jax.random.randint(jax.random.fold_in(rng, 1), (twos,), 0, 1 << 20) % (margin + 1)
    tallies = tallies.at[1:1 + 2 * twos:2].set(giver - moved).at[2:2 + 2 * twos:2].set(taker + moved)
    return tallies[jax.random.permutation(jax.random.fold_in(rng, 2), amount)]


def normal_values(own_key, extent, scale, most, shards=(), held_as=jnp.bfloat16):
    loudness = shard_levels(own_key, extent, shards, -0.22, 0.18) if shards else 1.0
    array = jax.random.normal(own_key, extent, jnp.float32) * scale * loudness
    return jnp.minimum(jnp.maximum(array, -most), most).astype(held_as)


def setup_inputs(seed: int = 0, part: int = 0) -> dict:
    key_list = jax.random.split(jax.random.key(seed), 12)
    own_keys = jax.random.split(jax.random.fold_in(key_list[11], part), 12)
    hidden = draw_hidden(jax.random.fold_in(jax.random.fold_in(key_list[11], part), 71), part)
    segment_ids = jnp.searchsorted(jnp.cumsum(uneven_parts(own_keys[1], SEGMENTS, LENGTH, 3 * LENGTH // 4, 1)), jnp.arange(LENGTH), side="right").astype(jnp.int32)
    targets = touch_ends(skewed_ids(own_keys[2], (LENGTH,), VOCAB, 2), jax.random.fold_in(own_keys[2], 3), 0, VOCAB - 1).astype(jnp.int32)
    loss_mask = draw_loss_mask(jax.random.fold_in(jax.random.fold_in(key_list[11], part), 71), part)
    attn_gain = jnp.clip(jnp.exp(math.log(2.0) - 1.3862944 * jax.random.uniform(key_list[4], (2, D), jnp.float32) ** shard_levels(key_list[4], (2, D), ((0, 2),), -0.2, 0.2)), 0.5, 2.0)
    final_gain = jnp.clip(jnp.exp(math.log(4.0) - 1.3862944 * jax.random.uniform(key_list[5], (2, D), jnp.float32) ** shard_levels(key_list[5], (2, D), ((0, 2),), -0.2, 0.2)), 1.0, 4.0)
    w_query = draw_w_query(jax.random.fold_in(key_list[11], 71), part)
    w_key = draw_w_key(jax.random.fold_in(key_list[11], 71), part)
    w_value = normal_values(key_list[8], (2, D, KV_HEADS * HEAD_DIM), D ** -0.5, 0.09375, ((0, 2), (1, 4), (2, 2)))
    w_out = normal_values(key_list[9], (2, HEADS * HEAD_DIM, D), (HEADS * HEAD_DIM) ** -0.5, 0.125, ((0, 2), (1, 2), (2, 4)))
    head = draw_head(jax.random.fold_in(key_list[11], 71), part)
    return dict(hidden=hidden, segment_ids=segment_ids, targets=targets, loss_mask=loss_mask, attn_gain=attn_gain, final_gain=final_gain, w_query=w_query, w_key=w_key, w_value=w_value, w_out=w_out, head=head)


EPS = 1e-05
THETA = 500000.0

def rms_norm(values, gain):
    return values * lax.rsqrt(lax.optimization_barrier(jnp.mean(values * values, axis=-1, keepdims=True)) + EPS) * gain

def rotate(tensor, offsets):
    half = tensor.shape[-1] // 2
    freq = THETA ** (-(jnp.arange(half, dtype=jnp.float32) * 2.0 / tensor.shape[-1]))
    angle = offsets.astype(jnp.float32)[:, None] * freq[None, :]
    cosine = jnp.cos(angle)[:, None, :]
    sine = jnp.sin(angle)[:, None, :]
    first = tensor[..., :half]
    second = tensor[..., half:]
    return jnp.concatenate([first * cosine - second * sine, second * cosine + first * sine], axis=-1)

def one_model(x, gain_a, gain_f, wq, wk, wv, wo, table, segment_ids, targets, loss_mask):
    length = x.shape[0]
    position = jnp.arange(length, dtype=jnp.int32)
    labels = jnp.arange(SEGMENTS, dtype=jnp.int32)
    member = segment_ids[None, :] == labels[:, None]
    starts = lax.optimization_barrier(jnp.min(jnp.where(member, position[None, :], length), axis=1)).astype(jnp.int32)
    token_start = lax.optimization_barrier(jnp.sum(jnp.where(member, starts[:, None], 0), axis=0)).astype(jnp.int32)
    offsets = position - token_start
    xfloat = x.astype(jnp.float32)
    normed = rms_norm(xfloat, gain_a).astype(jnp.bfloat16)
    keys = jnp.dot(normed, wk, preferred_element_type=jnp.float32).reshape(length, KV_HEADS, HEAD_DIM)
    keys = rotate(keys, offsets).astype(jnp.bfloat16)
    values = jnp.dot(normed, wv, preferred_element_type=jnp.float32).reshape(length, KV_HEADS, HEAD_DIM).astype(jnp.bfloat16)
    blocks = length // TOK_DEV
    mask_blocks = loss_mask.reshape(blocks, TOK_DEV)
    ranking = jnp.cumsum(mask_blocks, axis=1) - 1
    picks = (mask_blocks[:, None, :] == 1) & (ranking[:, None, :] == jnp.arange(CAP, dtype=jnp.int32)[None, :, None])
    inside = jnp.arange(TOK_DEV, dtype=jnp.int32)
    row_pos = lax.optimization_barrier(jnp.sum(jnp.where(picks, inside[None, None, :], 0), axis=2)) + (jnp.arange(blocks, dtype=jnp.int32) * TOK_DEV)[:, None]
    row_pos = row_pos.reshape(-1).astype(jnp.int32)
    valid = jnp.any(picks, axis=2).reshape(-1)
    rows = row_pos.shape[0]
    query = jnp.dot(normed[row_pos], wq, preferred_element_type=jnp.float32).reshape(rows, HEADS, HEAD_DIM)
    query = rotate(query, offsets[row_pos]).astype(jnp.bfloat16)
    front = jnp.zeros((WINDOW, KV_HEADS, HEAD_DIM), jnp.bfloat16)
    key_pad = jnp.concatenate([front, keys], axis=0)
    value_pad = jnp.concatenate([front, values], axis=0)
    group = HEADS // KV_HEADS
    scale = HEAD_DIM ** (-0.5)

    def attend(inputs):
        qrow, where_at, begin = inputs
        kslice = lax.dynamic_slice_in_dim(key_pad, where_at + 1, WINDOW, 0)
        vslice = lax.dynamic_slice_in_dim(value_pad, where_at + 1, WINDOW, 0)
        kpos = where_at - WINDOW + 1 + jnp.arange(WINDOW, dtype=jnp.int32)
        allowed = kpos >= begin
        grouped = qrow.astype(jnp.float32).reshape(KV_HEADS, group, HEAD_DIM)
        scores = jnp.einsum('ngd,knd->ngk', grouped, kslice.astype(jnp.float32)) * scale
        scores = jnp.where(allowed[None, None, :], scores, -1e+30)
        top = lax.optimization_barrier(jnp.max(scores, axis=-1, keepdims=True))
        expo = jnp.exp(scores - top)
        weights = (expo / lax.optimization_barrier(jnp.sum(expo, axis=-1, keepdims=True))).astype(jnp.bfloat16)
        out = jnp.einsum('ngk,knd->ngd', weights.astype(jnp.float32), vslice.astype(jnp.float32))
        return out.astype(jnp.bfloat16).reshape(HEADS * HEAD_DIM)
    attended = lax.map(attend, (query, row_pos, token_start[row_pos]))
    projected = jnp.dot(attended, wo, preferred_element_type=jnp.float32)
    state = xfloat[row_pos] + projected
    final = rms_norm(state, gain_f).astype(jnp.bfloat16)
    logits = jnp.dot(final, table, preferred_element_type=jnp.float32)
    top = lax.optimization_barrier(jnp.max(logits, axis=1))
    total = lax.optimization_barrier(jnp.sum(jnp.exp(logits - top[:, None]), axis=1))
    picked = jnp.take_along_axis(logits, targets[row_pos][:, None], axis=1)[:, 0]
    result = jnp.where(valid, picked - (top + jnp.log(total)), 0.0)
    return jnp.zeros((length,), jnp.float32).at[row_pos].add(result)

def reference(hidden, segment_ids, targets, loss_mask, attn_gain, final_gain, w_query, w_key, w_value, w_out, head):
    outputs = []
    for model in range(2):
        outputs.append(one_model(hidden[model], attn_gain[model], final_gain[model], w_query[model], w_key[model], w_value[model], w_out[model], head[model], segment_ids, targets, loss_mask))
    return jnp.stack(outputs)
```

```python
import functools

import jax
import jax.numpy as jnp
from jax import lax
from jax.experimental import pallas as pl
from jax.experimental.pallas import tpu as pltpu
from jax.sharding import PartitionSpec as P

HEAD_DIM = 128
WINDOW = 2048
CAP = 32
SEGMENTS = 4


EPS = 1e-05
THETA = 500000.0
FARTHEST = 1073741824


def passed_along(value, axis, by):
    length = lax.axis_size(axis)
    pairs = [(i, i + by) for i in range(length) if 0 <= i + by < length]
    return lax.ppermute(value, axis, pairs)


def joined(part, axis, combine):
    gathered = jax.tree.map(lambda a: lax.all_gather(a, axis), part)

    def take(source):
        return jax.tree.map(lambda a: lax.dynamic_index_in_dim(a, source, 0, False), gathered)

    return lax.fori_loop(
        1, lax.axis_size(axis), lambda source, state: combine(state, take(source)), take(0)
    )


def rms_norm(values, gain):
    return values * lax.rsqrt(jnp.mean(values * values, axis=-1, keepdims=True) + EPS) * gain


def rotate(tensor, offsets):
    half = tensor.shape[-1] // 2
    freq = THETA ** (-(jnp.arange(half, dtype=jnp.float32) * 2.0 / tensor.shape[-1]))
    angle = offsets.astype(jnp.float32)[:, None] * freq[None, :]
    cosine = jnp.cos(angle)[:, None, :]
    sine = jnp.sin(angle)[:, None, :]
    first = tensor[..., :half]
    second = tensor[..., half:]
    return jnp.concatenate(
        [first * cosine - second * sine, second * cosine + first * sine], axis=-1
    )


def combine_stats(left, right):
    top = jnp.maximum(left[0], right[0])
    total = left[1] * jnp.exp(left[0] - top) + right[1] * jnp.exp(right[0] - top)
    return (top, total, left[2] + right[2])


def block_stats(scores, allowed):
    row_peak = jnp.max(scores, axis=-1)
    lifted = jnp.where(allowed[None, None, :, :], jnp.exp(scores - row_peak[..., None]), 0.0)
    return (row_peak, jnp.sum(lifted, axis=-1))


def weighted_values(scores, row_peak, row_total, value_block):
    safe_total = jnp.where(row_total > 0.0, row_total, 1.0)
    weights = (jnp.exp(scores - row_peak[..., None]) / safe_total[..., None]).astype(jnp.bfloat16)
    return jnp.einsum("ngck,knd->cngd", weights, value_block, preferred_element_type=jnp.float32)


def gathered_weights(
    hidden,
    segment_ids,
    targets,
    loss_mask,
    attn_gain,
    final_gain,
    w_query,
    w_key,
    w_value,
    w_out,
    head,
):
    tokens = hidden.shape[1]
    seq_index = lax.axis_index("seq")
    base = seq_index * tokens
    position = base + jnp.arange(tokens, dtype=jnp.int32)
    whole = lax.all_gather(hidden[0], "tp", axis=1, tiled=True)
    xfloat = whole.astype(jnp.float32)
    normed = rms_norm(xfloat, attn_gain[0]).astype(jnp.bfloat16)
    labels = jnp.arange(SEGMENTS, dtype=jnp.int32)
    member = segment_ids[None, :] == labels[:, None]
    local_first = jnp.min(jnp.where(member, position[None, :], FARTHEST), axis=1)
    starts = lax.pmin(local_first, "seq")
    token_start = jnp.sum(jnp.where(member, starts[:, None], 0), axis=0)
    offsets = position - token_start
    ranking = jnp.cumsum(loss_mask) - 1
    picks = (loss_mask[None, :] == 1) & (
        ranking[None, :] == jnp.arange(CAP, dtype=jnp.int32)[:, None]
    )
    chooser = picks.astype(jnp.bfloat16)
    normed_rows = jnp.dot(chooser, normed, preferred_element_type=jnp.float32).astype(jnp.bfloat16)
    x_rows = jnp.dot(chooser, whole, preferred_element_type=jnp.float32)
    row_pos = jnp.sum(jnp.where(picks, position[None, :], 0), axis=1)
    row_start = jnp.sum(jnp.where(picks, token_start[None, :], 0), axis=1)
    row_target = jnp.sum(jnp.where(picks, targets[None, :], 0), axis=1)
    places = jnp.stack([row_pos, row_start])
    query_cols = w_query.shape[2]
    key_cols = w_key.shape[2]
    local_heads = query_cols // HEAD_DIM
    local_kv = key_cols // HEAD_DIM
    group = local_heads // local_kv
    score_scale = HEAD_DIM ** (-0.5)
    query = jnp.dot(
        normed_rows,
        lax.all_gather(w_query[0], "seq", axis=0, tiled=True),
        preferred_element_type=jnp.float32,
    )
    keys = jnp.dot(
        normed,
        lax.all_gather(w_key[0], "seq", axis=0, tiled=True),
        preferred_element_type=jnp.float32,
    )
    values = jnp.dot(
        normed,
        lax.all_gather(w_value[0], "seq", axis=0, tiled=True),
        preferred_element_type=jnp.float32,
    )
    query = rotate(query.reshape(CAP, local_heads, HEAD_DIM), row_pos - row_start).astype(
        jnp.bfloat16
    )
    keys = rotate(keys.reshape(tokens, local_kv, HEAD_DIM), offsets).astype(jnp.bfloat16)
    values = values.reshape(tokens, local_kv, HEAD_DIM).astype(jnp.bfloat16)

    def masked_scores(query_rows, bounds, key_block, key_base):
        key_pos = key_base + jnp.arange(key_block.shape[0], dtype=jnp.int32)
        row_at = bounds[0][:, None]
        allowed = (key_pos[None, :] <= row_at) & (row_at - key_pos[None, :] < WINDOW)
        allowed = allowed & (key_pos[None, :] >= bounds[1][:, None])
        grouped = query_rows.reshape(CAP, local_kv, group, HEAD_DIM)
        scores = (
            jnp.einsum("cngd,knd->ngck", grouped, key_block, preferred_element_type=jnp.float32)
            * score_scale
        )
        return (jnp.where(allowed[None, None, :, :], scores, -1e30), allowed)

    reach = min(WINDOW // tokens, lax.axis_size("seq") - 1)
    own_scores, own_allowed = masked_scores(query, places, keys, base)
    row_peak, row_total = block_stats(own_scores, own_allowed)
    visited = []
    for step in range(1, reach + 1):
        guest = passed_along(query, "seq", -step)
        guest_places = passed_along(places, "seq", -step)
        guest_scores, guest_allowed = masked_scores(guest, guest_places, keys, base)
        guest_peak, guest_total = block_stats(guest_scores, guest_allowed)
        returned = passed_along(jnp.stack([guest_peak, guest_total]), "seq", step)
        back_peak = jnp.where(seq_index >= step, returned[0], -1e30)
        merged_peak = jnp.maximum(row_peak, back_peak)
        row_total = row_total * jnp.exp(row_peak - merged_peak) + returned[1] * jnp.exp(
            back_peak - merged_peak
        )
        row_peak = merged_peak
        visited.append(guest_scores)
    attended = weighted_values(own_scores, row_peak, row_total, values)
    for step in range(1, reach + 1):
        guest_stats = passed_along(jnp.stack([row_peak, row_total]), "seq", -step)
        share = weighted_values(visited[step - 1], guest_stats[0], guest_stats[1], values)
        attended = attended + passed_along(share, "seq", step)
    attended = attended.astype(jnp.bfloat16).reshape(CAP, query_cols)
    partial_out = jnp.dot(
        attended,
        lax.all_gather(w_out[0], "seq", axis=1, tiled=True),
        preferred_element_type=jnp.float32,
    )
    summed = lax.psum(partial_out, "tp")
    state = x_rows + summed
    final = rms_norm(state, final_gain[0]).astype(jnp.bfloat16)
    all_rows = lax.all_gather(final, "seq", axis=0, tiled=True)
    all_targets = lax.all_gather(row_target, "seq", axis=0, tiled=True)
    logits = jnp.dot(all_rows, head[0], preferred_element_type=jnp.float32)
    vocab_start = (seq_index * lax.axis_size("tp") + lax.axis_index("tp")) * head.shape[2]
    local_top = jnp.max(logits, axis=1)
    local_total = jnp.sum(jnp.exp(logits - local_top[:, None]), axis=1)
    hit = all_targets[:, None] == vocab_start + jnp.arange(head.shape[2], dtype=jnp.int32)[None, :]
    local_target = jnp.sum(jnp.where(hit, logits, 0.0), axis=1)
    merged_top, merged_total, merged_target = joined(
        (local_top, local_total, local_target), ("seq", "tp"), combine_stats
    )
    logp = merged_target - (merged_top + jnp.log(merged_total))
    own = lax.dynamic_slice_in_dim(logp, seq_index * CAP, CAP, 0)
    placed = jnp.sum(jnp.where(picks, own[:, None], 0.0), axis=0)
    return placed[None, :].astype(jnp.float32)


def place():
    return lax.axis_index("seq"), lax.axis_index("tp")


def greet(peers):
    barrier = pltpu.get_barrier_semaphore()
    for peer in peers:
        pl.semaphore_signal(barrier, inc=1, device_id=peer, device_id_type=pl.DeviceIdType.MESH)
    pl.semaphore_wait(barrier, len(peers))


def remote(source, target, send, recv, peer):
    return pltpu.make_async_remote_copy(
        src_ref=source,
        dst_ref=target,
        send_sem=send,
        recv_sem=recv,
        device_id=peer,
        device_id_type=pl.DeviceIdType.MESH,
    )


def everyone(seq, tp):
    s, t = place()
    return [
        ((d, e), {"seq": lax.rem(s + d, seq), "tp": lax.rem(t + e, tp)})
        for d in range(seq)
        for e in range(tp)
        if (d, e) != (0, 0)
    ]


def tell_all(seq, tp, value, out, send, recv):
    s, t = place()
    out[s, t] = value[...]
    copies = []
    for number, (_, peer) in enumerate(everyone(seq, tp)):
        copy = remote(value, out.at[s, t], send.at[number], recv.at[number], peer)
        copy.start()
        copies.append(copy)
    return copies


def spread_kernel(seq, big, meta, out, told, half, send, recv, fsend, frecv, msend, mrecv, xsend, xrecv):
    s, t = place()
    other = 1 - t
    width = out.shape[-1]
    per = seq // 2
    greet([peer for _, peer in everyone(seq, 2)])
    beside = {"seq": s, "tp": other}
    first = remote(big.at[other], half, xsend, xrecv, beside)
    first.start()
    messages = tell_all(seq, 2, meta, told, msend, mrecv)

    def blocks(base, view):
        for i in range(per):
            target = base * per + i

            @pl.when(target != s)
            def _():
                remote(
                    view(i), out.at[s, t], send.at[base * per + i], recv.at[s], {"seq": target, "tp": t}
                ).start()

            @pl.when(target == s)
            def _():
                remote(view(i), out.at[s, t], fsend.at[s], frecv.at[s], beside).start()
                out[s, t] = view(i)[...]

    own = lambda i: big.at[t, :, pl.ds(i * width, width)]
    got = lambda i: half.at[:, pl.ds(i * width, width)]
    blocks(t, own)
    first.wait_recv()
    blocks(other, got)
    for d in (1, seq - 1, *range(2, seq - 1)):
        source = lax.rem(s + d, seq)
        remote(out.at[source, t], out.at[source, t], send.at[source], recv.at[source], beside).wait_recv()
        remote(out.at[source, t], out.at[source, t], fsend.at[source], frecv.at[source], beside).start()
    first.wait_send()
    for d in range(seq):
        source = lax.rem(s + d, seq)
        if d:
            remote(own(0), out.at[s, t], send.at[source], recv.at[source], beside).wait_send()
        remote(out.at[source, t], out.at[source, other], fsend.at[source], frecv.at[source], beside).wait()
    for copy in messages:
        copy.wait()


def spread(big, meta, seq, width):
    rows = big.shape[1]
    return pl.pallas_call(
        functools.partial(spread_kernel, seq),
        out_shape=(
            jax.ShapeDtypeStruct((seq, 2, rows, width), jnp.bfloat16),
            jax.ShapeDtypeStruct((seq, 2) + meta.shape, jnp.float32),
        ),
        in_specs=[pl.BlockSpec(memory_space=pltpu.VMEM)] * 2,
        out_specs=[pl.BlockSpec(memory_space=pltpu.VMEM)] * 2,
        scratch_shapes=[pltpu.VMEM(big.shape[1:], jnp.bfloat16)]
        + [pltpu.SemaphoreType.DMA((seq,))] * 4
        + [pltpu.SemaphoreType.DMA((2 * seq,))] * 2
        + [pltpu.SemaphoreType.DMA] * 2,
        compiler_params=pltpu.CompilerParams(collective_id=0, has_side_effects=True),
    )(big, meta)


def scatter_kernel(seq, count, *refs):
    parts, outs, (send, recv) = refs[:count], refs[count : 2 * count], refs[2 * count :]
    s, t = place()
    greet([{"seq": lax.rem(s + d, seq), "tp": t} for d in range(1, seq)])
    copies = []
    for d in (2, *range(1, 2), *range(3, seq)):
        target = lax.rem(s + d, seq)
        for number, (part, out) in enumerate(zip(parts, outs)):
            width = out.shape[-1]
            columns = pl.ds(pl.multiple_of(target * width, width), width)
            copy = remote(
                part.at[:, columns],
                out.at[d],
                send.at[d, number],
                recv.at[d, number],
                {"seq": target, "tp": t},
            )
            copy.start()
            copies.append(copy)
    for part, out in zip(parts, outs):
        width = out.shape[-1]
        out[0] = part[:, pl.ds(pl.multiple_of(s * width, width), width)]
    for copy in copies:
        copy.wait()


def scatter(parts, seq):
    count = len(parts)
    return pl.pallas_call(
        functools.partial(scatter_kernel, seq, count),
        out_shape=tuple(
            jax.ShapeDtypeStruct((seq, p.shape[0], p.shape[1] // seq), p.dtype) for p in parts
        ),
        in_specs=[pl.BlockSpec(memory_space=pltpu.VMEM)] * count,
        out_specs=[pl.BlockSpec(memory_space=pltpu.VMEM)] * count,
        scratch_shapes=[pltpu.SemaphoreType.DMA((seq, count))] * 2,
        compiler_params=pltpu.CompilerParams(collective_id=1, has_side_effects=True),
    )(*parts)


def heads_kernel(seq, part, out, send, recv):
    s, t = place()
    width = part.shape[1]
    greet([{"seq": lax.rem(s + d, seq), "tp": t} for d in range(1, seq)])
    mine = pl.ds(pl.multiple_of(s * width, width), width)
    copies = []
    for d in range(1, seq):
        copy = remote(
            part, out.at[:, mine], send.at[d], recv.at[d], {"seq": lax.rem(s + d, seq), "tp": t}
        )
        copy.start()
        copies.append(copy)
    out[:, mine] = part[...]
    for copy in copies:
        copy.wait()


def gather_heads(part, seq):
    return pl.pallas_call(
        functools.partial(heads_kernel, seq),
        out_shape=jax.ShapeDtypeStruct((part.shape[0], part.shape[1] * seq), part.dtype),
        in_specs=[pl.BlockSpec(memory_space=pltpu.VMEM)],
        out_specs=pl.BlockSpec(memory_space=pltpu.VMEM),
        scratch_shapes=[pltpu.SemaphoreType.DMA((seq,))] * 2,
        compiler_params=pltpu.CompilerParams(collective_id=2, has_side_effects=True),
    )(part)


def rows_kernel(seq, part, squares, out, told, send, recv, fsend, frecv, msend, mrecv):
    s, t = place()
    rows, width = part.shape
    greet([peer for _, peer in everyone(seq, 2)])
    beside = {"seq": s, "tp": 1 - t}

    def spot(source, half):
        return out.at[
            pl.ds(pl.multiple_of(half * rows, rows), rows),
            pl.ds(pl.multiple_of(source * width, width), width),
        ]

    copies = []
    for d in (2, 1, 3)[: seq - 1]:
        copy = remote(part, spot(s, t), send.at[d], recv.at[d], {"seq": lax.rem(s + d, seq), "tp": t})
        copy.start()
        copies.append((d, copy))
    aside = remote(part, spot(s, t), fsend.at[0], frecv.at[0], beside)
    aside.start()
    forwards = [aside]
    messages = tell_all(seq, 2, squares, told, msend, mrecv)
    spot(s, t)[...] = part[...]
    for d, copy in copies[1:] + copies[:1]:
        copy.wait_recv()
        source = lax.rem(s - d + seq, seq)
        forward = remote(spot(source, t), spot(source, t), fsend.at[d], frecv.at[d], beside)
        forward.start()
        forwards.append(forward)
    for _, copy in copies:
        copy.wait_send()
    for copy in forwards + messages:
        copy.wait()


def gather_rows(part, squares, seq):
    rows, width = part.shape
    return pl.pallas_call(
        functools.partial(rows_kernel, seq),
        out_shape=(
            jax.ShapeDtypeStruct((2 * rows, width * seq), part.dtype),
            jax.ShapeDtypeStruct((seq, 2) + squares.shape, jnp.float32),
        ),
        in_specs=[pl.BlockSpec(memory_space=pltpu.VMEM)] * 2,
        out_specs=[pl.BlockSpec(memory_space=pltpu.VMEM)] * 2,
        scratch_shapes=[pltpu.SemaphoreType.DMA((seq,))] * 4
        + [pltpu.SemaphoreType.DMA((2 * seq,))] * 2,
        compiler_params=pltpu.CompilerParams(collective_id=3, has_side_effects=True),
    )(part, squares)


def stats_kernel(seq, stats, told, send, recv):
    greet([peer for _, peer in everyone(seq, 2)])
    for copy in tell_all(seq, 2, stats, told, send, recv):
        copy.wait()


def gather_stats(stats, seq):
    return pl.pallas_call(
        functools.partial(stats_kernel, seq),
        out_shape=jax.ShapeDtypeStruct((seq, 2) + stats.shape, jnp.float32),
        in_specs=[pl.BlockSpec(memory_space=pltpu.VMEM)],
        out_specs=pl.BlockSpec(memory_space=pltpu.VMEM),
        scratch_shapes=[pltpu.SemaphoreType.DMA((2 * seq,))] * 2,
        compiler_params=pltpu.CompilerParams(collective_id=4, has_side_effects=True),
    )(stats)


def padded(rows, lanes):
    stacked = jnp.stack([r.astype(jnp.float32) for r in rows])
    return jnp.pad(stacked, ((0, 8 - len(rows)), (0, lanes - stacked.shape[1])))


def picks_of(mask):
    ranking = jnp.cumsum(mask, axis=-1) - 1
    return (mask[..., None, :] == 1) & (
        ranking[..., None, :] == jnp.arange(CAP, dtype=jnp.int32)[:, None]
    )


def moved_rows(
    hidden,
    segment_ids,
    targets,
    loss_mask,
    attn_gain,
    final_gain,
    w_query,
    w_key,
    w_value,
    w_out,
    head,
):
    seq = lax.axis_size("seq")
    s, t = place()
    tokens, features = hidden.shape[1:]
    model = features * 2
    width = w_key.shape[1]
    length = seq * tokens
    x = hidden[0]
    xfloat = x.astype(jnp.float32)
    gain = lax.dynamic_slice_in_dim(attn_gain[0], t * features, features)
    scaled = (xfloat * gain).astype(jnp.bfloat16)
    squares = jnp.sum(xfloat * xfloat, axis=1)
    chooser = picks_of(loss_mask).astype(jnp.bfloat16)
    pick_scaled = jnp.dot(chooser, scaled, preferred_element_type=jnp.float32).astype(jnp.bfloat16)
    pick_raw = jnp.dot(chooser, x, preferred_element_type=jnp.float32).astype(jnp.bfloat16)
    big = jnp.concatenate(
        [
            scaled.reshape(2, tokens // 2, features),
            pick_scaled.reshape(2, CAP // 2, features),
            pick_raw.reshape(2, CAP // 2, features),
        ],
        axis=1,
    )
    meta = padded([segment_ids, loss_mask, targets, squares], tokens)
    spread_out, told = spread(big, meta, seq, width)

    half = tokens // 2
    token_block = spread_out[:, :, :half].reshape(length, width)
    row_block = spread_out[:, :, half : half + CAP // 2].reshape(seq * CAP, width)
    raw_block = spread_out[:, :, half + CAP // 2 :].reshape(seq * CAP, width)
    key_part = jnp.dot(token_block, w_key[0], preferred_element_type=jnp.float32)
    value_part = jnp.dot(token_block, w_value[0], preferred_element_type=jnp.float32)
    query_part = jnp.dot(row_block, w_query[0], preferred_element_type=jnp.float32)

    keys, values, query = scatter(
        [p.astype(jnp.bfloat16) for p in (key_part, value_part, query_part)], seq
    )

    whole = told[:, 0].astype(jnp.int32)
    segments = whole[:, 0].reshape(length)
    masks = whole[:, 1]
    position = jnp.arange(length, dtype=jnp.int32)
    member = segments[None, :] == jnp.arange(SEGMENTS, dtype=jnp.int32)[:, None]
    starts = jnp.min(jnp.where(member, position[None, :], FARTHEST), axis=1)
    token_start = jnp.sum(jnp.where(member, starts[:, None], 0), axis=0)
    offsets = position - token_start
    scale = lax.rsqrt((told[:, 0, 3] + told[:, 1, 3]) / model + EPS)
    picks = picks_of(masks)

    def chosen(values):
        return jnp.sum(jnp.where(picks, values.reshape(seq, 1, tokens), 0), axis=2).reshape(-1)

    row_pos = chosen(position)
    row_start = chosen(token_start)
    row_target = chosen(whole[:, 2])
    row_scale = chosen(scale)

    def total(parts):
        return jnp.sum(parts.astype(jnp.float32), axis=0)

    key_all = total(keys) * scale.reshape(length, 1)
    value_all = (total(values) * scale.reshape(length, 1)).astype(jnp.bfloat16)
    query_all = total(query) * row_scale[:, None]
    group = query_all.shape[1] // HEAD_DIM
    key_all = rotate(key_all[:, None, :], offsets)[:, 0].astype(jnp.bfloat16)
    query_all = rotate(query_all.reshape(seq * CAP, group, HEAD_DIM), row_pos - row_start).astype(
        jnp.bfloat16
    )
    allowed = (position[None, :] <= row_pos[:, None]) & (position[None, :] >= row_start[:, None])
    allowed = allowed & (row_pos[:, None] - position[None, :] < WINDOW)
    scores = jnp.einsum("cgd,kd->gck", query_all, key_all, preferred_element_type=jnp.float32)
    scores = jnp.where(allowed[None], scores * HEAD_DIM ** (-0.5), -1e30)
    peak = jnp.max(scores, axis=-1, keepdims=True)
    lifted = jnp.exp(scores - peak)
    weights = (lifted / jnp.sum(lifted, axis=-1, keepdims=True)).astype(jnp.bfloat16)
    attended = jnp.einsum("gck,kd->cgd", weights, value_all, preferred_element_type=jnp.float32)
    attended = attended.astype(jnp.bfloat16).reshape(seq * CAP, group * HEAD_DIM)
    attended = gather_heads(attended, seq)
    partial_out = jnp.dot(attended, w_out[0], preferred_element_type=jnp.float32)

    rows = seq * CAP // 2
    away = lax.dynamic_slice_in_dim(partial_out, (1 - t) * rows, rows).astype(jnp.bfloat16)
    here = lax.dynamic_slice_in_dim(partial_out, t * rows, rows)
    here = here + lax.dynamic_slice_in_dim(raw_block, t * rows, rows).astype(jnp.float32)
    state = here + lax.ppermute(away, "tp", [(0, 1), (1, 0)]).astype(jnp.float32)
    late_gain = lax.dynamic_slice_in_dim(final_gain[0], s * width, width)
    late = (state * late_gain).astype(jnp.bfloat16)
    final, late_squares = gather_rows(late, padded([jnp.sum(state * state, axis=1)], 128), seq)
    late_mean = jnp.sum(late_squares[:, :, 0, :rows], axis=0).reshape(-1) / model
    logits = jnp.dot(final, head[0], preferred_element_type=jnp.float32)
    logits = logits * lax.rsqrt(late_mean + EPS)[:, None]
    entries = head.shape[2]
    first_entry = (s * 2 + t) * entries
    top = jnp.max(logits, axis=1)
    exps = jnp.sum(jnp.exp(logits - top[:, None]), axis=1)
    hit = row_target[:, None] == first_entry + jnp.arange(entries, dtype=jnp.int32)[None, :]
    found = jnp.sum(jnp.where(hit, logits, 0.0), axis=1)
    stats = gather_stats(padded([top, exps, found], seq * CAP), seq)
    mine = lax.dynamic_slice_in_dim(stats.reshape(seq * 2, 8, seq * CAP), s * CAP, CAP, 2)
    best = jnp.max(mine[:, 0], axis=0)
    summed = jnp.sum(mine[:, 1] * jnp.exp(mine[:, 0] - best[None, :]), axis=0)
    logp = jnp.sum(mine[:, 2], axis=0) - (best + jnp.log(summed))
    placed = jnp.sum(jnp.where(picks_of(loss_mask), logp[:, None], 0.0), axis=0)
    return placed[None, :].astype(jnp.float32)


def solution(mesh):
    placed = (
        P("ref", ("groups", "seq"), "tp"),
        P(("groups", "seq")),
        P(("groups", "seq")),
        P(("groups", "seq")),
        P("ref", None),
        P("ref", None),
        P("ref", "seq", "tp"),
        P("ref", "seq", "tp"),
        P("ref", "seq", "tp"),
        P("ref", "tp", "seq"),
        P("ref", None, ("seq", "tp")),
    )

    def shards(*args):
        seq, tp = mesh.shape["seq"], mesh.shape["tp"]
        own_heads = args[7].shape[2] // HEAD_DIM
        moves = tp == 2 and seq == 4 and own_heads % seq == 0
        return (moved_rows if moves else gathered_weights)(*args)

    return jax.shard_map(
        shards, mesh=mesh, in_specs=placed, out_specs=P("ref", ("groups", "seq")), check_vma=False
    )
```

```python
import functools

import jax
import jax.numpy as jnp
from jax import lax
from jax.experimental import pallas as pl
from jax.experimental.pallas import tpu as pltpu
from jax.sharding import PartitionSpec as P

HEAD_DIM = 128
WINDOW = 2048
CAP = 32
SEGMENTS = 4


EPS = 1e-05
THETA = 500000.0
FARTHEST = 1073741824


def passed_along(value, axis, by):
    length = lax.axis_size(axis)
    pairs = [(i, i + by) for i in range(length) if 0 <= i + by < length]
    return lax.ppermute(value, axis, pairs)


def joined(part, axis, combine):
    gathered = jax.tree.map(lambda a: lax.all_gather(a, axis), part)

    def take(source):
        return jax.tree.map(lambda a: lax.dynamic_index_in_dim(a, source, 0, False), gathered)

    return lax.fori_loop(
        1, lax.axis_size(axis), lambda source, state: combine(state, take(source)), take(0)
    )


def rms_norm(values, gain):
    return values * lax.rsqrt(jnp.mean(values * values, axis=-1, keepdims=True) + EPS) * gain


def rotate(tensor, offsets):
    half = tensor.shape[-1] // 2
    freq = THETA ** (-(jnp.arange(half, dtype=jnp.float32) * 2.0 / tensor.shape[-1]))
    angle = offsets.astype(jnp.float32)[:, None] * freq[None, :]
    cosine = jnp.cos(angle)[:, None, :]
    sine = jnp.sin(angle)[:, None, :]
    first = tensor[..., :half]
    second = tensor[..., half:]
    return jnp.concatenate(
        [first * cosine - second * sine, second * cosine + first * sine], axis=-1
    )


def combine_stats(left, right):
    top = jnp.maximum(left[0], right[0])
    total = left[1] * jnp.exp(left[0] - top) + right[1] * jnp.exp(right[0] - top)
    return (top, total, left[2] + right[2])


def block_stats(scores, allowed):
    row_peak = jnp.max(scores, axis=-1)
    lifted = jnp.where(allowed[None, None, :, :], jnp.exp(scores - row_peak[..., None]), 0.0)
    return (row_peak, jnp.sum(lifted, axis=-1))


def weighted_values(scores, row_peak, row_total, value_block):
    safe_total = jnp.where(row_total > 0.0, row_total, 1.0)
    weights = (jnp.exp(scores - row_peak[..., None]) / safe_total[..., None]).astype(jnp.bfloat16)
    return jnp.einsum("ngck,knd->cngd", weights, value_block, preferred_element_type=jnp.float32)


def gathered_weights(
    hidden,
    segment_ids,
    targets,
    loss_mask,
    attn_gain,
    final_gain,
    w_query,
    w_key,
    w_value,
    w_out,
    head,
):
    tokens = hidden.shape[1]
    seq_index = lax.axis_index("seq")
    base = seq_index * tokens
    position = base + jnp.arange(tokens, dtype=jnp.int32)
    whole = lax.all_gather(hidden[0], "tp", axis=1, tiled=True)
    xfloat = whole.astype(jnp.float32)
    normed = rms_norm(xfloat, attn_gain[0]).astype(jnp.bfloat16)
    labels = jnp.arange(SEGMENTS, dtype=jnp.int32)
    member = segment_ids[None, :] == labels[:, None]
    local_first = jnp.min(jnp.where(member, position[None, :], FARTHEST), axis=1)
    starts = lax.pmin(local_first, "seq")
    token_start = jnp.sum(jnp.where(member, starts[:, None], 0), axis=0)
    offsets = position - token_start
    ranking = jnp.cumsum(loss_mask) - 1
    picks = (loss_mask[None, :] == 1) & (
        ranking[None, :] == jnp.arange(CAP, dtype=jnp.int32)[:, None]
    )
    chooser = picks.astype(jnp.bfloat16)
    normed_rows = jnp.dot(chooser, normed, preferred_element_type=jnp.float32).astype(jnp.bfloat16)
    x_rows = jnp.dot(chooser, whole, preferred_element_type=jnp.float32)
    row_pos = jnp.sum(jnp.where(picks, position[None, :], 0), axis=1)
    row_start = jnp.sum(jnp.where(picks, token_start[None, :], 0), axis=1)
    row_target = jnp.sum(jnp.where(picks, targets[None, :], 0), axis=1)
    places = jnp.stack([row_pos, row_start])
    query_cols = w_query.shape[2]
    key_cols = w_key.shape[2]
    local_heads = query_cols // HEAD_DIM
    local_kv = key_cols // HEAD_DIM
    group = local_heads // local_kv
    score_scale = HEAD_DIM ** (-0.5)
    query = jnp.dot(
        normed_rows,
        lax.all_gather(w_query[0], "seq", axis=0, tiled=True),
        preferred_element_type=jnp.float32,
    )
    keys = jnp.dot(
        normed,
        lax.all_gather(w_key[0], "seq", axis=0, tiled=True),
        preferred_element_type=jnp.float32,
    )
    values = jnp.dot(
        normed,
        lax.all_gather(w_value[0], "seq", axis=0, tiled=True),
        preferred_element_type=jnp.float32,
    )
    query = rotate(query.reshape(CAP, local_heads, HEAD_DIM), row_pos - row_start).astype(
        jnp.bfloat16
    )
    keys = rotate(keys.reshape(tokens, local_kv, HEAD_DIM), offsets).astype(jnp.bfloat16)
    values = values.reshape(tokens, local_kv, HEAD_DIM).astype(jnp.bfloat16)

    def masked_scores(query_rows, bounds, key_block, key_base):
        key_pos = key_base + jnp.arange(key_block.shape[0], dtype=jnp.int32)
        row_at = bounds[0][:, None]
        allowed = (key_pos[None, :] <= row_at) & (row_at - key_pos[None, :] < WINDOW)
        allowed = allowed & (key_pos[None, :] >= bounds[1][:, None])
        grouped = query_rows.reshape(CAP, local_kv, group, HEAD_DIM)
        scores = (
            jnp.einsum("cngd,knd->ngck", grouped, key_block, preferred_element_type=jnp.float32)
            * score_scale
        )
        return (jnp.where(allowed[None, None, :, :], scores, -1e30), allowed)

    reach = min(WINDOW // tokens, lax.axis_size("seq") - 1)
    own_scores, own_allowed = masked_scores(query, places, keys, base)
    row_peak, row_total = block_stats(own_scores, own_allowed)
    visited = []
    for step in range(1, reach + 1):
        guest = passed_along(query, "seq", -step)
        guest_places = passed_along(places, "seq", -step)
        guest_scores, guest_allowed = masked_scores(guest, guest_places, keys, base)
        guest_peak, guest_total = block_stats(guest_scores, guest_allowed)
        returned = passed_along(jnp.stack([guest_peak, guest_total]), "seq", step)
        back_peak = jnp.where(seq_index >= step, returned[0], -1e30)
        merged_peak = jnp.maximum(row_peak, back_peak)
        row_total = row_total * jnp.exp(row_peak - merged_peak) + returned[1] * jnp.exp(
            back_peak - merged_peak
        )
        row_peak = merged_peak
        visited.append(guest_scores)
    attended = weighted_values(own_scores, row_peak, row_total, values)
    for step in range(1, reach + 1):
        guest_stats = passed_along(jnp.stack([row_peak, row_total]), "seq", -step)
        share = weighted_values(visited[step - 1], guest_stats[0], guest_stats[1], values)
        attended = attended + passed_along(share, "seq", step)
    attended = attended.astype(jnp.bfloat16).reshape(CAP, query_cols)
    partial_out = jnp.dot(
        attended,
        lax.all_gather(w_out[0], "seq", axis=1, tiled=True),
        preferred_element_type=jnp.float32,
    )
    summed = lax.psum(partial_out, "tp")
    state = x_rows + summed
    final = rms_norm(state, final_gain[0]).astype(jnp.bfloat16)
    all_rows = lax.all_gather(final, "seq", axis=0, tiled=True)
    all_targets = lax.all_gather(row_target, "seq", axis=0, tiled=True)
    logits = jnp.dot(all_rows, head[0], preferred_element_type=jnp.float32)
    vocab_start = (seq_index * lax.axis_size("tp") + lax.axis_index("tp")) * head.shape[2]
    local_top = jnp.max(logits, axis=1)
    local_total = jnp.sum(jnp.exp(logits - local_top[:, None]), axis=1)
    hit = all_targets[:, None] == vocab_start + jnp.arange(head.shape[2], dtype=jnp.int32)[None, :]
    local_target = jnp.sum(jnp.where(hit, logits, 0.0), axis=1)
    merged_top, merged_total, merged_target = joined(
        (local_top, local_total, local_target), ("seq", "tp"), combine_stats
    )
    logp = merged_target - (merged_top + jnp.log(merged_total))
    own = lax.dynamic_slice_in_dim(logp, seq_index * CAP, CAP, 0)
    placed = jnp.sum(jnp.where(picks, own[:, None], 0.0), axis=0)
    return placed[None, :].astype(jnp.float32)


def place():
    return lax.axis_index("seq"), lax.axis_index("tp")


def greet(peers):
    barrier = pltpu.get_barrier_semaphore()
    for peer in peers:
        pl.semaphore_signal(barrier, inc=1, device_id=peer, device_id_type=pl.DeviceIdType.MESH)
    pl.semaphore_wait(barrier, len(peers))


def remote(source, target, send, recv, peer):
    return pltpu.make_async_remote_copy(
        src_ref=source,
        dst_ref=target,
        send_sem=send,
        recv_sem=recv,
        device_id=peer,
        device_id_type=pl.DeviceIdType.MESH,
    )


def everyone(seq, tp):
    s, t = place()
    return [
        ((d, e), {"seq": lax.rem(s + d, seq), "tp": lax.rem(t + e, tp)})
        for d in range(seq)
        for e in range(tp)
        if (d, e) != (0, 0)
    ]


def tell_all(seq, tp, value, out, send, recv):
    s, t = place()
    out[s, t] = value[...]
    copies = []
    for number, (_, peer) in enumerate(everyone(seq, tp)):
        copy = remote(value, out.at[s, t], send.at[number], recv.at[number], peer)
        copy.start()
        copies.append(copy)
    return copies


def project_kernel(
    seq,
    pick,
    big,
    meta,
    w_query,
    w_key,
    w_value,
    out,
    raw,
    told,
    half,
    blocks,
    parts,
    send,
    recv,
    fsend,
    frecv,
    msend,
    mrecv,
    psend,
    precv,
    xsend,
    xrecv,
):
    s, t = place()
    other = 1 - t
    width = blocks.shape[-1]
    tokens = blocks.shape[2] - 2 * pick
    per = seq // 2
    greet([peer for _, peer in everyone(seq, 2)])
    beside = {"seq": s, "tp": other}
    first = remote(big.at[other], half, xsend, xrecv, beside)
    first.start()
    messages = tell_all(seq, 2, meta, told, msend, mrecv)

    def hand_out(base, view):
        for i in range(per):
            target = base * per + i

            @pl.when(target != s)
            def _():
                remote(
                    view(i),
                    blocks.at[s, t],
                    send.at[target],
                    recv.at[s],
                    {"seq": target, "tp": t},
                ).start()

            @pl.when(target == s)
            def _():
                remote(view(i), blocks.at[s, t], fsend.at[s], frecv.at[s], beside).start()
                blocks[s, t] = view(i)[...]

    own = lambda i: big.at[t, :, pl.ds(i * width, width)]
    got = lambda i: half.at[:, pl.ds(i * width, width)]
    hand_out(t, own)
    first.wait_recv()
    hand_out(other, got)

    def arrived(source):
        return remote(
            blocks.at[source, t], blocks.at[source, t], send.at[source], recv.at[source], beside
        )

    def passed(source):
        return remote(
            blocks.at[source, t], blocks.at[source, t], fsend.at[source], frecv.at[source], beside
        )

    def handed(chunk, d):
        return remote(
            parts.at[chunk, d],
            out.at[d, chunk],
            psend.at[chunk, d],
            precv.at[chunk, d],
            {"seq": lax.rem(s + d, seq), "tp": t},
        )

    def project(source, side):
        chunk = source * 2 + side
        rows = blocks[source, side, :tokens]
        chosen = blocks[source, side, tokens : tokens + pick]
        raw[source, side] = blocks[source, side, tokens + pick :]
        dot = functools.partial(jnp.dot, preferred_element_type=jnp.float32)
        for d in range(seq):
            target = lax.rem(s + d, seq)
            single = pl.ds(pl.multiple_of(target * HEAD_DIM, HEAD_DIM), HEAD_DIM)
            wide = out.shape[-1]
            double = pl.ds(pl.multiple_of(target * wide, wide), wide)
            place_at = out.at[0, chunk] if d == 0 else parts.at[chunk, d]
            place_at[:tokens, :HEAD_DIM] = dot(rows, w_key[:, single]).astype(jnp.bfloat16)
            place_at[:tokens, HEAD_DIM:] = dot(rows, w_value[:, single]).astype(jnp.bfloat16)
            place_at[tokens:] = dot(chosen, w_query[:, double]).astype(jnp.bfloat16)
        for d in (2, 1, 3):
            handed(chunk, d).start()

    side_of = s // 2
    partner = s + 1 - 2 * lax.rem(s, 2)

    def step(number, carry):
        source = jnp.where(
            number == 0,
            s,
            jnp.where(
                number == 1, partner, jnp.where(number == 2, 2 - side_of, 3 * (1 - side_of))
            ),
        )

        @pl.when(number > 0)
        def _():
            arrived(source).wait_recv()
            passed(source).start()

        def both(side, more):
            which = lax.rem(t + side, 2)

            @pl.when(side == 1)
            def _():
                passed(source).wait_recv()

            project(source, which)
            return more

        return lax.fori_loop(0, 2, both, carry)

    lax.fori_loop(0, seq, step, 0)
    first.wait_send()
    for source in range(seq):

        @pl.when(source != s)
        def _():
            arrived(source).wait_send()

        passed(source).wait_send()
    for copy in messages:
        copy.wait()
    for d in range(1, seq):
        for chunk in range(2 * seq):
            handed(chunk, d).wait()


def project(big, meta, w_query, w_key, w_value, seq, pick):
    rows = big.shape[1]
    width = w_key.shape[0]
    wide = w_query.shape[1] // seq
    return pl.pallas_call(
        functools.partial(project_kernel, seq, pick),
        out_shape=(
            jax.ShapeDtypeStruct((seq, 2 * seq, rows - pick, wide), jnp.bfloat16),
            jax.ShapeDtypeStruct((seq, 2, pick, width), jnp.bfloat16),
            jax.ShapeDtypeStruct((seq, 2) + meta.shape, jnp.float32),
        ),
        in_specs=[pl.BlockSpec(memory_space=pltpu.VMEM)] * 5,
        out_specs=[pl.BlockSpec(memory_space=pltpu.VMEM)] * 3,
        scratch_shapes=[
            pltpu.VMEM(big.shape[1:], jnp.bfloat16),
            pltpu.VMEM((seq, 2, rows, width), jnp.bfloat16),
            pltpu.VMEM((2 * seq, seq, rows - pick, wide), jnp.bfloat16),
        ]
        + [pltpu.SemaphoreType.DMA((seq,))] * 4
        + [pltpu.SemaphoreType.DMA((2 * seq,))] * 2
        + [pltpu.SemaphoreType.DMA((2 * seq, seq))] * 2
        + [pltpu.SemaphoreType.DMA] * 2,
        compiler_params=pltpu.CompilerParams(collective_id=0, has_side_effects=True),
    )(big, meta, w_query, w_key, w_value)


def heads_kernel(seq, part, out, send, recv):
    s, t = place()
    width = part.shape[1]
    greet([{"seq": lax.rem(s + d, seq), "tp": t} for d in range(1, seq)])
    mine = pl.ds(pl.multiple_of(s * width, width), width)
    copies = []
    for d in range(1, seq):
        copy = remote(
            part, out.at[:, mine], send.at[d], recv.at[d], {"seq": lax.rem(s + d, seq), "tp": t}
        )
        copy.start()
        copies.append(copy)
    out[:, mine] = part[...]
    for copy in copies:
        copy.wait()


def gather_heads(part, seq):
    return pl.pallas_call(
        functools.partial(heads_kernel, seq),
        out_shape=jax.ShapeDtypeStruct((part.shape[0], part.shape[1] * seq), part.dtype),
        in_specs=[pl.BlockSpec(memory_space=pltpu.VMEM)],
        out_specs=pl.BlockSpec(memory_space=pltpu.VMEM),
        scratch_shapes=[pltpu.SemaphoreType.DMA((seq,))] * 2,
        compiler_params=pltpu.CompilerParams(collective_id=2, has_side_effects=True),
    )(part)


def rows_kernel(seq, part, squares, out, told, send, recv, fsend, frecv, msend, mrecv):
    s, t = place()
    rows, width = part.shape
    greet([peer for _, peer in everyone(seq, 2)])
    beside = {"seq": s, "tp": 1 - t}

    def spot(source, half):
        return out.at[
            pl.ds(pl.multiple_of(half * rows, rows), rows),
            pl.ds(pl.multiple_of(source * width, width), width),
        ]

    copies = []
    for d in (2, 1, 3)[: seq - 1]:
        copy = remote(part, spot(s, t), send.at[d], recv.at[d], {"seq": lax.rem(s + d, seq), "tp": t})
        copy.start()
        copies.append((d, copy))
    aside = remote(part, spot(s, t), fsend.at[0], frecv.at[0], beside)
    aside.start()
    forwards = [aside]
    messages = tell_all(seq, 2, squares, told, msend, mrecv)
    spot(s, t)[...] = part[...]
    for d, copy in copies[1:] + copies[:1]:
        copy.wait_recv()
        source = lax.rem(s - d + seq, seq)
        forward = remote(spot(source, t), spot(source, t), fsend.at[d], frecv.at[d], beside)
        forward.start()
        forwards.append(forward)
    for _, copy in copies:
        copy.wait_send()
    for copy in forwards + messages:
        copy.wait()


def gather_rows(part, squares, seq):
    rows, width = part.shape
    return pl.pallas_call(
        functools.partial(rows_kernel, seq),
        out_shape=(
            jax.ShapeDtypeStruct((2 * rows, width * seq), part.dtype),
            jax.ShapeDtypeStruct((seq, 2) + squares.shape, jnp.float32),
        ),
        in_specs=[pl.BlockSpec(memory_space=pltpu.VMEM)] * 2,
        out_specs=[pl.BlockSpec(memory_space=pltpu.VMEM)] * 2,
        scratch_shapes=[pltpu.SemaphoreType.DMA((seq,))] * 4
        + [pltpu.SemaphoreType.DMA((2 * seq,))] * 2,
        compiler_params=pltpu.CompilerParams(collective_id=3, has_side_effects=True),
    )(part, squares)


def stats_kernel(seq, stats, told, send, recv):
    greet([peer for _, peer in everyone(seq, 2)])
    for copy in tell_all(seq, 2, stats, told, send, recv):
        copy.wait()


def gather_stats(stats, seq):
    return pl.pallas_call(
        functools.partial(stats_kernel, seq),
        out_shape=jax.ShapeDtypeStruct((seq, 2) + stats.shape, jnp.float32),
        in_specs=[pl.BlockSpec(memory_space=pltpu.VMEM)],
        out_specs=pl.BlockSpec(memory_space=pltpu.VMEM),
        scratch_shapes=[pltpu.SemaphoreType.DMA((2 * seq,))] * 2,
        compiler_params=pltpu.CompilerParams(collective_id=4, has_side_effects=True),
    )(stats)


def padded(rows, lanes):
    stacked = jnp.stack([r.astype(jnp.float32) for r in rows])
    return jnp.pad(stacked, ((0, 8 - len(rows)), (0, lanes - stacked.shape[1])))


def picks_of(mask):
    ranking = jnp.cumsum(mask, axis=-1) - 1
    return (mask[..., None, :] == 1) & (
        ranking[..., None, :] == jnp.arange(CAP, dtype=jnp.int32)[:, None]
    )


def moved_rows(
    hidden,
    segment_ids,
    targets,
    loss_mask,
    attn_gain,
    final_gain,
    w_query,
    w_key,
    w_value,
    w_out,
    head,
):
    seq = lax.axis_size("seq")
    s, t = place()
    tokens, features = hidden.shape[1:]
    model = features * 2
    width = w_key.shape[1]
    length = seq * tokens
    x = hidden[0]
    xfloat = x.astype(jnp.float32)
    gain = lax.dynamic_slice_in_dim(attn_gain[0], t * features, features)
    scaled = (xfloat * gain).astype(jnp.bfloat16)
    squares = jnp.sum(xfloat * xfloat, axis=1)
    chooser = picks_of(loss_mask).astype(jnp.bfloat16)
    pick_scaled = jnp.dot(chooser, scaled, preferred_element_type=jnp.float32).astype(jnp.bfloat16)
    pick_raw = jnp.dot(chooser, x, preferred_element_type=jnp.float32).astype(jnp.bfloat16)
    big = jnp.concatenate(
        [
            scaled.reshape(2, tokens // 2, features),
            pick_scaled.reshape(2, CAP // 2, features),
            pick_raw.reshape(2, CAP // 2, features),
        ],
        axis=1,
    )
    meta = padded([segment_ids, loss_mask, targets, squares], tokens)
    parts, raw, told = project(big, meta, w_query[0], w_key[0], w_value[0], seq, CAP // 2)
    half = tokens // 2
    raw_block = raw.reshape(seq * CAP, width)

    whole = told[:, 0].astype(jnp.int32)
    segments = whole[:, 0].reshape(length)
    masks = whole[:, 1]
    position = jnp.arange(length, dtype=jnp.int32)
    member = segments[None, :] == jnp.arange(SEGMENTS, dtype=jnp.int32)[:, None]
    starts = jnp.min(jnp.where(member, position[None, :], FARTHEST), axis=1)
    token_start = jnp.sum(jnp.where(member, starts[:, None], 0), axis=0)
    offsets = position - token_start
    scale = lax.rsqrt((told[:, 0, 3] + told[:, 1, 3]) / model + EPS)
    picks = picks_of(masks)

    def chosen(values):
        return jnp.sum(jnp.where(picks, values.reshape(seq, 1, tokens), 0), axis=2).reshape(-1)

    row_pos = chosen(position)
    row_start = chosen(token_start)
    row_target = chosen(whole[:, 2])
    row_scale = chosen(scale)

    summed = jnp.sum(parts.astype(jnp.float32), axis=0)
    key_all = summed[:, :half, :HEAD_DIM].reshape(length, HEAD_DIM) * scale.reshape(length, 1)
    value_all = summed[:, :half, HEAD_DIM:].reshape(length, HEAD_DIM) * scale.reshape(length, 1)
    value_all = value_all.astype(jnp.bfloat16)
    query_all = summed[:, half:].reshape(seq * CAP, -1) * row_scale[:, None]
    group = query_all.shape[1] // HEAD_DIM
    key_all = rotate(key_all[:, None, :], offsets)[:, 0].astype(jnp.bfloat16)
    query_all = rotate(query_all.reshape(seq * CAP, group, HEAD_DIM), row_pos - row_start).astype(
        jnp.bfloat16
    )
    allowed = (position[None, :] <= row_pos[:, None]) & (position[None, :] >= row_start[:, None])
    allowed = allowed & (row_pos[:, None] - position[None, :] < WINDOW)
    scores = jnp.einsum("cgd,kd->gck", query_all, key_all, preferred_element_type=jnp.float32)
    scores = jnp.where(allowed[None], scores * HEAD_DIM ** (-0.5), -1e30)
    peak = jnp.max(scores, axis=-1, keepdims=True)
    lifted = jnp.exp(scores - peak)
    weights = (lifted / jnp.sum(lifted, axis=-1, keepdims=True)).astype(jnp.bfloat16)
    attended = jnp.einsum("gck,kd->cgd", weights, value_all, preferred_element_type=jnp.float32)
    attended = attended.astype(jnp.bfloat16).reshape(seq * CAP, group * HEAD_DIM)
    attended = gather_heads(attended, seq)
    partial_out = jnp.dot(attended, w_out[0], preferred_element_type=jnp.float32)

    rows = seq * CAP // 2
    away = lax.dynamic_slice_in_dim(partial_out, (1 - t) * rows, rows).astype(jnp.bfloat16)
    here = lax.dynamic_slice_in_dim(partial_out, t * rows, rows)
    here = here + lax.dynamic_slice_in_dim(raw_block, t * rows, rows).astype(jnp.float32)
    state = here + lax.ppermute(away, "tp", [(0, 1), (1, 0)]).astype(jnp.float32)
    late_gain = lax.dynamic_slice_in_dim(final_gain[0], s * width, width)
    late = (state * late_gain).astype(jnp.bfloat16)
    final, late_squares = gather_rows(late, padded([jnp.sum(state * state, axis=1)], 128), seq)
    late_mean = jnp.sum(late_squares[:, :, 0, :rows], axis=0).reshape(-1) / model
    logits = jnp.dot(final, head[0], preferred_element_type=jnp.float32)
    logits = logits * lax.rsqrt(late_mean + EPS)[:, None]
    entries = head.shape[2]
    first_entry = (s * 2 + t) * entries
    top = jnp.max(logits, axis=1)
    exps = jnp.sum(jnp.exp(logits - top[:, None]), axis=1)
    hit = row_target[:, None] == first_entry + jnp.arange(entries, dtype=jnp.int32)[None, :]
    found = jnp.sum(jnp.where(hit, logits, 0.0), axis=1)
    stats = gather_stats(padded([top, exps, found], seq * CAP), seq)
    mine = lax.dynamic_slice_in_dim(stats.reshape(seq * 2, 8, seq * CAP), s * CAP, CAP, 2)
    best = jnp.max(mine[:, 0], axis=0)
    summed = jnp.sum(mine[:, 1] * jnp.exp(mine[:, 0] - best[None, :]), axis=0)
    logp = jnp.sum(mine[:, 2], axis=0) - (best + jnp.log(summed))
    placed = jnp.sum(jnp.where(picks_of(loss_mask), logp[:, None], 0.0), axis=0)
    return placed[None, :].astype(jnp.float32)


def solution(mesh):
    placed = (
        P("ref", ("groups", "seq"), "tp"),
        P(("groups", "seq")),
        P(("groups", "seq")),
        P(("groups", "seq")),
        P("ref", None),
        P("ref", None),
        P("ref", "seq", "tp"),
        P("ref", "seq", "tp"),
        P("ref", "seq", "tp"),
        P("ref", "tp", "seq"),
        P("ref", None, ("seq", "tp")),
    )

    def shards(*args):
        seq, tp = mesh.shape["seq"], mesh.shape["tp"]
        own_heads = args[7].shape[2] // HEAD_DIM
        moves = tp == 2 and seq == 4 and own_heads == seq and args[6].shape[2] == 2 * args[7].shape[2]
        return (moved_rows if moves else gathered_weights)(*args)

    return jax.shard_map(
        shards, mesh=mesh, in_specs=placed, out_specs=P("ref", ("groups", "seq")), check_vma=False
    )
```

```python
import functools

import jax
import jax.numpy as jnp
from jax import lax
from jax.experimental import pallas as pl
from jax.experimental.pallas import tpu as pltpu
from jax.sharding import PartitionSpec as P

HEAD_DIM = 128
WINDOW = 2048
CAP = 32
SEGMENTS = 4


EPS = 1e-05
THETA = 500000.0
FARTHEST = 1073741824


def passed_along(value, axis, by):
    length = lax.axis_size(axis)
    pairs = [(i, i + by) for i in range(length) if 0 <= i + by < length]
    return lax.ppermute(value, axis, pairs)


def joined(part, axis, combine):
    gathered = jax.tree.map(lambda a: lax.all_gather(a, axis), part)

    def take(source):
        return jax.tree.map(lambda a: lax.dynamic_index_in_dim(a, source, 0, False), gathered)

    return lax.fori_loop(
        1, lax.axis_size(axis), lambda source, state: combine(state, take(source)), take(0)
    )


def rms_norm(values, gain):
    return values * lax.rsqrt(jnp.mean(values * values, axis=-1, keepdims=True) + EPS) * gain


def rotate(tensor, offsets):
    half = tensor.shape[-1] // 2
    freq = THETA ** (-(jnp.arange(half, dtype=jnp.float32) * 2.0 / tensor.shape[-1]))
    angle = offsets.astype(jnp.float32)[:, None] * freq[None, :]
    cosine = jnp.cos(angle)[:, None, :]
    sine = jnp.sin(angle)[:, None, :]
    first = tensor[..., :half]
    second = tensor[..., half:]
    return jnp.concatenate(
        [first * cosine - second * sine, second * cosine + first * sine], axis=-1
    )


def combine_stats(left, right):
    top = jnp.maximum(left[0], right[0])
    total = left[1] * jnp.exp(left[0] - top) + right[1] * jnp.exp(right[0] - top)
    return (top, total, left[2] + right[2])


def block_stats(scores, allowed):
    row_peak = jnp.max(scores, axis=-1)
    lifted = jnp.where(allowed[None, None, :, :], jnp.exp(scores - row_peak[..., None]), 0.0)
    return (row_peak, jnp.sum(lifted, axis=-1))


def weighted_values(scores, row_peak, row_total, value_block):
    safe_total = jnp.where(row_total > 0.0, row_total, 1.0)
    weights = (jnp.exp(scores - row_peak[..., None]) / safe_total[..., None]).astype(jnp.bfloat16)
    return jnp.einsum("ngck,knd->cngd", weights, value_block, preferred_element_type=jnp.float32)


def gathered_weights(
    hidden,
    segment_ids,
    targets,
    loss_mask,
    attn_gain,
    final_gain,
    w_query,
    w_key,
    w_value,
    w_out,
    head,
):
    tokens = hidden.shape[1]
    seq_index = lax.axis_index("seq")
    base = seq_index * tokens
    position = base + jnp.arange(tokens, dtype=jnp.int32)
    whole = lax.all_gather(hidden[0], "tp", axis=1, tiled=True)
    xfloat = whole.astype(jnp.float32)
    normed = rms_norm(xfloat, attn_gain[0]).astype(jnp.bfloat16)
    labels = jnp.arange(SEGMENTS, dtype=jnp.int32)
    member = segment_ids[None, :] == labels[:, None]
    local_first = jnp.min(jnp.where(member, position[None, :], FARTHEST), axis=1)
    starts = lax.pmin(local_first, "seq")
    token_start = jnp.sum(jnp.where(member, starts[:, None], 0), axis=0)
    offsets = position - token_start
    ranking = jnp.cumsum(loss_mask) - 1
    picks = (loss_mask[None, :] == 1) & (
        ranking[None, :] == jnp.arange(CAP, dtype=jnp.int32)[:, None]
    )
    chooser = picks.astype(jnp.bfloat16)
    normed_rows = jnp.dot(chooser, normed, preferred_element_type=jnp.float32).astype(jnp.bfloat16)
    x_rows = jnp.dot(chooser, whole, preferred_element_type=jnp.float32)
    row_pos = jnp.sum(jnp.where(picks, position[None, :], 0), axis=1)
    row_start = jnp.sum(jnp.where(picks, token_start[None, :], 0), axis=1)
    row_target = jnp.sum(jnp.where(picks, targets[None, :], 0), axis=1)
    places = jnp.stack([row_pos, row_start])
    query_cols = w_query.shape[2]
    key_cols = w_key.shape[2]
    local_heads = query_cols // HEAD_DIM
    local_kv = key_cols // HEAD_DIM
    group = local_heads // local_kv
    score_scale = HEAD_DIM ** (-0.5)
    query = jnp.dot(
        normed_rows,
        lax.all_gather(w_query[0], "seq", axis=0, tiled=True),
        preferred_element_type=jnp.float32,
    )
    keys = jnp.dot(
        normed,
        lax.all_gather(w_key[0], "seq", axis=0, tiled=True),
        preferred_element_type=jnp.float32,
    )
    values = jnp.dot(
        normed,
        lax.all_gather(w_value[0], "seq", axis=0, tiled=True),
        preferred_element_type=jnp.float32,
    )
    query = rotate(query.reshape(CAP, local_heads, HEAD_DIM), row_pos - row_start).astype(
        jnp.bfloat16
    )
    keys = rotate(keys.reshape(tokens, local_kv, HEAD_DIM), offsets).astype(jnp.bfloat16)
    values = values.reshape(tokens, local_kv, HEAD_DIM).astype(jnp.bfloat16)

    def masked_scores(query_rows, bounds, key_block, key_base):
        key_pos = key_base + jnp.arange(key_block.shape[0], dtype=jnp.int32)
        row_at = bounds[0][:, None]
        allowed = (key_pos[None, :] <= row_at) & (row_at - key_pos[None, :] < WINDOW)
        allowed = allowed & (key_pos[None, :] >= bounds[1][:, None])
        grouped = query_rows.reshape(CAP, local_kv, group, HEAD_DIM)
        scores = (
            jnp.einsum("cngd,knd->ngck", grouped, key_block, preferred_element_type=jnp.float32)
            * score_scale
        )
        return (jnp.where(allowed[None, None, :, :], scores, -1e30), allowed)

    reach = min(WINDOW // tokens, lax.axis_size("seq") - 1)
    own_scores, own_allowed = masked_scores(query, places, keys, base)
    row_peak, row_total = block_stats(own_scores, own_allowed)
    visited = []
    for step in range(1, reach + 1):
        guest = passed_along(query, "seq", -step)
        guest_places = passed_along(places, "seq", -step)
        guest_scores, guest_allowed = masked_scores(guest, guest_places, keys, base)
        guest_peak, guest_total = block_stats(guest_scores, guest_allowed)
        returned = passed_along(jnp.stack([guest_peak, guest_total]), "seq", step)
        back_peak = jnp.where(seq_index >= step, returned[0], -1e30)
        merged_peak = jnp.maximum(row_peak, back_peak)
        row_total = row_total * jnp.exp(row_peak - merged_peak) + returned[1] * jnp.exp(
            back_peak - merged_peak
        )
        row_peak = merged_peak
        visited.append(guest_scores)
    attended = weighted_values(own_scores, row_peak, row_total, values)
    for step in range(1, reach + 1):
        guest_stats = passed_along(jnp.stack([row_peak, row_total]), "seq", -step)
        share = weighted_values(visited[step - 1], guest_stats[0], guest_stats[1], values)
        attended = attended + passed_along(share, "seq", step)
    attended = attended.astype(jnp.bfloat16).reshape(CAP, query_cols)
    partial_out = jnp.dot(
        attended,
        lax.all_gather(w_out[0], "seq", axis=1, tiled=True),
        preferred_element_type=jnp.float32,
    )
    summed = lax.psum(partial_out, "tp")
    state = x_rows + summed
    final = rms_norm(state, final_gain[0]).astype(jnp.bfloat16)
    all_rows = lax.all_gather(final, "seq", axis=0, tiled=True)
    all_targets = lax.all_gather(row_target, "seq", axis=0, tiled=True)
    logits = jnp.dot(all_rows, head[0], preferred_element_type=jnp.float32)
    vocab_start = (seq_index * lax.axis_size("tp") + lax.axis_index("tp")) * head.shape[2]
    local_top = jnp.max(logits, axis=1)
    local_total = jnp.sum(jnp.exp(logits - local_top[:, None]), axis=1)
    hit = all_targets[:, None] == vocab_start + jnp.arange(head.shape[2], dtype=jnp.int32)[None, :]
    local_target = jnp.sum(jnp.where(hit, logits, 0.0), axis=1)
    merged_top, merged_total, merged_target = joined(
        (local_top, local_total, local_target), ("seq", "tp"), combine_stats
    )
    logp = merged_target - (merged_top + jnp.log(merged_total))
    own = lax.dynamic_slice_in_dim(logp, seq_index * CAP, CAP, 0)
    placed = jnp.sum(jnp.where(picks, own[:, None], 0.0), axis=0)
    return placed[None, :].astype(jnp.float32)


def place():
    return lax.axis_index("seq"), lax.axis_index("tp")


def greet(peers):
    barrier = pltpu.get_barrier_semaphore()
    for peer in peers:
        pl.semaphore_signal(barrier, inc=1, device_id=peer, device_id_type=pl.DeviceIdType.MESH)
    pl.semaphore_wait(barrier, len(peers))


def remote(source, target, send, recv, peer):
    return pltpu.make_async_remote_copy(
        src_ref=source,
        dst_ref=target,
        send_sem=send,
        recv_sem=recv,
        device_id=peer,
        device_id_type=pl.DeviceIdType.MESH,
    )


def everyone(seq, tp):
    s, t = place()
    return [
        ((d, e), {"seq": lax.rem(s + d, seq), "tp": lax.rem(t + e, tp)})
        for d in range(seq)
        for e in range(tp)
        if (d, e) != (0, 0)
    ]


def tell_all(seq, tp, value, out, send, recv):
    s, t = place()
    out[s, t] = value[...]
    copies = []
    for number, (_, peer) in enumerate(everyone(seq, tp)):
        copy = remote(value, out.at[s, t], send.at[number], recv.at[number], peer)
        copy.start()
        copies.append(copy)
    return copies


def project_kernel(
    seq,
    pick,
    big,
    meta,
    w_query,
    w_key,
    w_value,
    out,
    raw,
    told,
    half,
    blocks,
    parts,
    joins,
    send,
    recv,
    fsend,
    frecv,
    msend,
    mrecv,
    psend,
    precv,
    xsend,
    xrecv,
):
    s, t = place()
    other = 1 - t
    width = blocks.shape[-1]
    tokens = blocks.shape[2] - 2 * pick
    per = seq // 2
    greet([peer for _, peer in everyone(seq, 2)])
    beside = {"seq": s, "tp": other}
    first = remote(big.at[other], half, xsend, xrecv, beside)
    first.start()
    messages = tell_all(seq, 2, meta, told, msend, mrecv)

    def hand_out(base, view):
        for i in range(per):
            target = base * per + i

            @pl.when(target != s)
            def _():
                remote(
                    view(i),
                    blocks.at[s, t],
                    send.at[target],
                    recv.at[s],
                    {"seq": target, "tp": t},
                ).start()

            @pl.when(target == s)
            def _():
                remote(view(i), blocks.at[s, t], fsend.at[s], frecv.at[s], beside).start()
                blocks[s, t] = view(i)[...]

    own = lambda i: big.at[t, :, pl.ds(i * width, width)]
    got = lambda i: half.at[:, pl.ds(i * width, width)]
    hand_out(t, own)
    first.wait_recv()
    hand_out(other, got)

    def arrived(source):
        return remote(
            blocks.at[source, t], blocks.at[source, t], send.at[source], recv.at[source], beside
        )

    def passed(source):
        return remote(
            blocks.at[source, t], blocks.at[source, t], fsend.at[source], frecv.at[source], beside
        )

    side_of = s // 2
    partner = s + 1 - 2 * lax.rem(s, 2)
    toward = lax.rem(partner - s + seq, seq)

    def handed(chunk, kind):
        slot = (0, toward, 2, seq - toward)[kind]
        target = out.at[kind, chunk] if kind < 3 else joins.at[chunk]
        peer = lax.rem(s + 2, seq) if kind == 2 else partner
        return remote(
            parts.at[chunk, slot],
            target,
            psend.at[chunk, kind],
            precv.at[chunk, kind],
            {"seq": peer, "tp": t},
        )

    def combine(source):
        def one(side, carry):
            chunk = source * 2 + lax.rem(t + side, 2)
            handed(chunk, 3).wait_recv()
            both = parts[chunk, 2].astype(jnp.float32) + joins[chunk].astype(jnp.float32)
            parts[chunk, 2] = both.astype(jnp.bfloat16)
            handed(chunk, 2).start()
            return carry

        lax.fori_loop(0, 2, one, 0)

    def project(source, side):
        chunk = source * 2 + side
        rows = blocks[source, side, :tokens]
        chosen = blocks[source, side, tokens : tokens + pick]
        raw[source, side] = blocks[source, side, tokens + pick :]
        dot = functools.partial(jnp.dot, preferred_element_type=jnp.float32)
        for d in range(seq):
            target = lax.rem(s + d, seq)
            single = pl.ds(pl.multiple_of(target * HEAD_DIM, HEAD_DIM), HEAD_DIM)
            wide = out.shape[-1]
            double = pl.ds(pl.multiple_of(target * wide, wide), wide)
            place_at = out.at[0, chunk] if d == 0 else parts.at[chunk, d]
            place_at[:tokens, :HEAD_DIM] = dot(rows, w_key[:, single]).astype(jnp.bfloat16)
            place_at[:tokens, HEAD_DIM:] = dot(rows, w_value[:, single]).astype(jnp.bfloat16)
            place_at[tokens:] = dot(chosen, w_query[:, double]).astype(jnp.bfloat16)
        for kind in (3, 1):
            handed(chunk, kind).start()

    near, far = 2 - side_of, 3 * (1 - side_of)

    def choose(number, first, second, third, fourth):
        return jnp.where(
            number == 0,
            first,
            jnp.where(number == 1, second, jnp.where(number == 2, third, fourth)),
        )

    def step(number, carry):
        source = choose(number, s, partner, near, far)

        @pl.when(number > 0)
        def _():
            arrived(source).wait_recv()
            passed(source).start()

        def both(side, more):
            which = lax.rem(t + side, 2)

            @pl.when(side == 1)
            def _():
                passed(source).wait_recv()

            project(source, which)
            return more

        done = lax.fori_loop(0, 2, both, carry)

        @pl.when(number > 0)
        def _():
            combine(choose(number, s, partner, s, near))

        return done

    lax.fori_loop(0, seq, step, 0)
    combine(far)
    first.wait_send()
    for source in range(seq):

        @pl.when(source != s)
        def _():
            arrived(source).wait_send()

        passed(source).wait_send()
    for copy in messages:
        copy.wait()
    for chunk in range(2 * seq):
        for kind in (1, 2):
            handed(chunk, kind).wait()
        handed(chunk, 3).wait_send()


def project(big, meta, w_query, w_key, w_value, seq, pick):
    rows = big.shape[1]
    width = w_key.shape[0]
    wide = w_query.shape[1] // seq
    return pl.pallas_call(
        functools.partial(project_kernel, seq, pick),
        out_shape=(
            jax.ShapeDtypeStruct((3, 2 * seq, rows - pick, wide), jnp.bfloat16),
            jax.ShapeDtypeStruct((seq, 2, pick, width), jnp.bfloat16),
            jax.ShapeDtypeStruct((seq, 2) + meta.shape, jnp.float32),
        ),
        in_specs=[pl.BlockSpec(memory_space=pltpu.VMEM)] * 5,
        out_specs=[pl.BlockSpec(memory_space=pltpu.VMEM)] * 3,
        scratch_shapes=[
            pltpu.VMEM(big.shape[1:], jnp.bfloat16),
            pltpu.VMEM((seq, 2, rows, width), jnp.bfloat16),
            pltpu.VMEM((2 * seq, seq, rows - pick, wide), jnp.bfloat16),
            pltpu.VMEM((2 * seq, rows - pick, wide), jnp.bfloat16),
        ]
        + [pltpu.SemaphoreType.DMA((seq,))] * 4
        + [pltpu.SemaphoreType.DMA((2 * seq,))] * 2
        + [pltpu.SemaphoreType.DMA((2 * seq, seq))] * 2
        + [pltpu.SemaphoreType.DMA] * 2,
        compiler_params=pltpu.CompilerParams(collective_id=0, has_side_effects=True),
    )(big, meta, w_query, w_key, w_value)


def heads_kernel(seq, part, out, send, recv):
    s, t = place()
    width = part.shape[1]
    greet([{"seq": lax.rem(s + d, seq), "tp": t} for d in range(1, seq)])
    mine = pl.ds(pl.multiple_of(s * width, width), width)
    copies = []
    for d in range(1, seq):
        copy = remote(
            part, out.at[:, mine], send.at[d], recv.at[d], {"seq": lax.rem(s + d, seq), "tp": t}
        )
        copy.start()
        copies.append(copy)
    out[:, mine] = part[...]
    for copy in copies:
        copy.wait()


def gather_heads(part, seq):
    return pl.pallas_call(
        functools.partial(heads_kernel, seq),
        out_shape=jax.ShapeDtypeStruct((part.shape[0], part.shape[1] * seq), part.dtype),
        in_specs=[pl.BlockSpec(memory_space=pltpu.VMEM)],
        out_specs=pl.BlockSpec(memory_space=pltpu.VMEM),
        scratch_shapes=[pltpu.SemaphoreType.DMA((seq,))] * 2,
        compiler_params=pltpu.CompilerParams(collective_id=2, has_side_effects=True),
    )(part)


def rows_kernel(seq, part, squares, out, told, send, recv, fsend, frecv, msend, mrecv):
    s, t = place()
    rows, width = part.shape
    greet([peer for _, peer in everyone(seq, 2)])
    beside = {"seq": s, "tp": 1 - t}

    def spot(source, half):
        return out.at[
            pl.ds(pl.multiple_of(half * rows, rows), rows),
            pl.ds(pl.multiple_of(source * width, width), width),
        ]

    copies = []
    for d in (2, 1, 3)[: seq - 1]:
        copy = remote(part, spot(s, t), send.at[d], recv.at[d], {"seq": lax.rem(s + d, seq), "tp": t})
        copy.start()
        copies.append((d, copy))
    aside = remote(part, spot(s, t), fsend.at[0], frecv.at[0], beside)
    aside.start()
    forwards = [aside]
    messages = tell_all(seq, 2, squares, told, msend, mrecv)
    spot(s, t)[...] = part[...]
    for d, copy in copies[1:] + copies[:1]:
        copy.wait_recv()
        source = lax.rem(s - d + seq, seq)
        forward = remote(spot(source, t), spot(source, t), fsend.at[d], frecv.at[d], beside)
        forward.start()
        forwards.append(forward)
    for _, copy in copies:
        copy.wait_send()
    for copy in forwards + messages:
        copy.wait()


def gather_rows(part, squares, seq):
    rows, width = part.shape
    return pl.pallas_call(
        functools.partial(rows_kernel, seq),
        out_shape=(
            jax.ShapeDtypeStruct((2 * rows, width * seq), part.dtype),
            jax.ShapeDtypeStruct((seq, 2) + squares.shape, jnp.float32),
        ),
        in_specs=[pl.BlockSpec(memory_space=pltpu.VMEM)] * 2,
        out_specs=[pl.BlockSpec(memory_space=pltpu.VMEM)] * 2,
        scratch_shapes=[pltpu.SemaphoreType.DMA((seq,))] * 4
        + [pltpu.SemaphoreType.DMA((2 * seq,))] * 2,
        compiler_params=pltpu.CompilerParams(collective_id=3, has_side_effects=True),
    )(part, squares)


def stats_kernel(seq, stats, told, send, recv):
    greet([peer for _, peer in everyone(seq, 2)])
    for copy in tell_all(seq, 2, stats, told, send, recv):
        copy.wait()


def gather_stats(stats, seq):
    return pl.pallas_call(
        functools.partial(stats_kernel, seq),
        out_shape=jax.ShapeDtypeStruct((seq, 2) + stats.shape, jnp.float32),
        in_specs=[pl.BlockSpec(memory_space=pltpu.VMEM)],
        out_specs=pl.BlockSpec(memory_space=pltpu.VMEM),
        scratch_shapes=[pltpu.SemaphoreType.DMA((2 * seq,))] * 2,
        compiler_params=pltpu.CompilerParams(collective_id=4, has_side_effects=True),
    )(stats)


def padded(rows, lanes):
    stacked = jnp.stack([r.astype(jnp.float32) for r in rows])
    return jnp.pad(stacked, ((0, 8 - len(rows)), (0, lanes - stacked.shape[1])))


def picks_of(mask):
    ranking = jnp.cumsum(mask, axis=-1) - 1
    return (mask[..., None, :] == 1) & (
        ranking[..., None, :] == jnp.arange(CAP, dtype=jnp.int32)[:, None]
    )


def moved_rows(
    hidden,
    segment_ids,
    targets,
    loss_mask,
    attn_gain,
    final_gain,
    w_query,
    w_key,
    w_value,
    w_out,
    head,
):
    seq = lax.axis_size("seq")
    s, t = place()
    tokens, features = hidden.shape[1:]
    model = features * 2
    width = w_key.shape[1]
    length = seq * tokens
    x = hidden[0]
    xfloat = x.astype(jnp.float32)
    gain = lax.dynamic_slice_in_dim(attn_gain[0], t * features, features)
    scaled = (xfloat * gain).astype(jnp.bfloat16)
    squares = jnp.sum(xfloat * xfloat, axis=1)
    chooser = picks_of(loss_mask).astype(jnp.bfloat16)
    pick_scaled = jnp.dot(chooser, scaled, preferred_element_type=jnp.float32).astype(jnp.bfloat16)
    pick_raw = jnp.dot(chooser, x, preferred_element_type=jnp.float32).astype(jnp.bfloat16)
    big = jnp.concatenate(
        [
            scaled.reshape(2, tokens // 2, features),
            pick_scaled.reshape(2, CAP // 2, features),
            pick_raw.reshape(2, CAP // 2, features),
        ],
        axis=1,
    )
    meta = padded([segment_ids, loss_mask, targets, squares], tokens)
    parts, raw, told = project(big, meta, w_query[0], w_key[0], w_value[0], seq, CAP // 2)
    half = tokens // 2
    raw_block = raw.reshape(seq * CAP, width)

    whole = told[:, 0].astype(jnp.int32)
    segments = whole[:, 0].reshape(length)
    masks = whole[:, 1]
    position = jnp.arange(length, dtype=jnp.int32)
    member = segments[None, :] == jnp.arange(SEGMENTS, dtype=jnp.int32)[:, None]
    starts = jnp.min(jnp.where(member, position[None, :], FARTHEST), axis=1)
    token_start = jnp.sum(jnp.where(member, starts[:, None], 0), axis=0)
    offsets = position - token_start
    scale = lax.rsqrt((told[:, 0, 3] + told[:, 1, 3]) / model + EPS)
    picks = picks_of(masks)

    def chosen(values):
        return jnp.sum(jnp.where(picks, values.reshape(seq, 1, tokens), 0), axis=2).reshape(-1)

    row_pos = chosen(position)
    row_start = chosen(token_start)
    row_target = chosen(whole[:, 2])
    row_scale = chosen(scale)

    summed = jnp.sum(parts.astype(jnp.float32), axis=0)
    key_all = summed[:, :half, :HEAD_DIM].reshape(length, HEAD_DIM) * scale.reshape(length, 1)
    value_all = summed[:, :half, HEAD_DIM:].reshape(length, HEAD_DIM) * scale.reshape(length, 1)
    value_all = value_all.astype(jnp.bfloat16)
    query_all = summed[:, half:].reshape(seq * CAP, -1) * row_scale[:, None]
    group = query_all.shape[1] // HEAD_DIM
    key_all = rotate(key_all[:, None, :], offsets)[:, 0].astype(jnp.bfloat16)
    query_all = rotate(query_all.reshape(seq * CAP, group, HEAD_DIM), row_pos - row_start).astype(
        jnp.bfloat16
    )
    allowed = (position[None, :] <= row_pos[:, None]) & (position[None, :] >= row_start[:, None])
    allowed = allowed & (row_pos[:, None] - position[None, :] < WINDOW)
    scores = jnp.einsum("cgd,kd->gck", query_all, key_all, preferred_element_type=jnp.float32)
    scores = jnp.where(allowed[None], scores * HEAD_DIM ** (-0.5), -1e30)
    peak = jnp.max(scores, axis=-1, keepdims=True)
    lifted = jnp.exp(scores - peak)
    weights = (lifted / jnp.sum(lifted, axis=-1, keepdims=True)).astype(jnp.bfloat16)
    attended = jnp.einsum("gck,kd->cgd", weights, value_all, preferred_element_type=jnp.float32)
    attended = attended.astype(jnp.bfloat16).reshape(seq * CAP, group * HEAD_DIM)
    attended = gather_heads(attended, seq)
    partial_out = jnp.dot(attended, w_out[0], preferred_element_type=jnp.float32)

    rows = seq * CAP // 2
    away = lax.dynamic_slice_in_dim(partial_out, (1 - t) * rows, rows).astype(jnp.bfloat16)
    here = lax.dynamic_slice_in_dim(partial_out, t * rows, rows)
    here = here + lax.dynamic_slice_in_dim(raw_block, t * rows, rows).astype(jnp.float32)
    state = here + lax.ppermute(away, "tp", [(0, 1), (1, 0)]).astype(jnp.float32)
    late_gain = lax.dynamic_slice_in_dim(final_gain[0], s * width, width)
    late = (state * late_gain).astype(jnp.bfloat16)
    final, late_squares = gather_rows(late, padded([jnp.sum(state * state, axis=1)], 128), seq)
    late_mean = jnp.sum(late_squares[:, :, 0, :rows], axis=0).reshape(-1) / model
    logits = jnp.dot(final, head[0], preferred_element_type=jnp.float32)
    logits = logits * lax.rsqrt(late_mean + EPS)[:, None]
    entries = head.shape[2]
    first_entry = (s * 2 + t) * entries
    top = jnp.max(logits, axis=1)
    exps = jnp.sum(jnp.exp(logits - top[:, None]), axis=1)
    hit = row_target[:, None] == first_entry + jnp.arange(entries, dtype=jnp.int32)[None, :]
    found = jnp.sum(jnp.where(hit, logits, 0.0), axis=1)
    stats = gather_stats(padded([top, exps, found], seq * CAP), seq)
    mine = lax.dynamic_slice_in_dim(stats.reshape(seq * 2, 8, seq * CAP), s * CAP, CAP, 2)
    best = jnp.max(mine[:, 0], axis=0)
    summed = jnp.sum(mine[:, 1] * jnp.exp(mine[:, 0] - best[None, :]), axis=0)
    logp = jnp.sum(mine[:, 2], axis=0) - (best + jnp.log(summed))
    placed = jnp.sum(jnp.where(picks_of(loss_mask), logp[:, None], 0.0), axis=0)
    return placed[None, :].astype(jnp.float32)


def solution(mesh):
    placed = (
        P("ref", ("groups", "seq"), "tp"),
        P(("groups", "seq")),
        P(("groups", "seq")),
        P(("groups", "seq")),
        P("ref", None),
        P("ref", None),
        P("ref", "seq", "tp"),
        P("ref", "seq", "tp"),
        P("ref", "seq", "tp"),
        P("ref", "tp", "seq"),
        P("ref", None, ("seq", "tp")),
    )

    def shards(*args):
        seq, tp = mesh.shape["seq"], mesh.shape["tp"]
        own_heads = args[7].shape[2] // HEAD_DIM
        moves = tp == 2 and seq == 4 and own_heads == seq and args[6].shape[2] == 2 * args[7].shape[2]
        return (moved_rows if moves else gathered_weights)(*args)

    return jax.shard_map(
        shards, mesh=mesh, in_specs=placed, out_specs=P("ref", ("groups", "seq")), check_vma=False
    )
```
